32 devices in a mesh: slab: 8 (over z, y), md: 4 (over x, core).
Axes of the slice: x: 2, y: 2, z: 4, core: 2. Of those that a mesh axis runs over, the one named last changes fastest.
Arguments:
- populations: float32 [19, 16, 256, 128], P(None, 'slab', 'md'), may hold values from 0.02 to 0.1
- relax: float32 [16, 256, 128], P('slab', 'md'), may hold values from 0.8 to 1.8
- owners: int32 [16, 256, 2], P('slab', 'md'), may hold values from 0 to 31, all different within a row; in each aligned block of 64 rows (0 to 63, 64 to 127, ..., all dimensions but the last counted through in order) at most 8 rows name the same one
- positions: float32 [3, 32768], P(None, ('slab', 'md')), may hold values from 0 to 3
- velocities: float32 [3, 32768], P(None, ('slab', 'md')), may hold values from -5 to 5
- neighbours: int32 [32768, 64], P(('slab', 'md')), may hold values from 0 to 1023
- atom_slots: int32 [32768], P(('slab', 'md')), may hold values from 0 to 511
Outputs:
- populations_out: float32 [19, 16, 256, 128], P(None, 'slab', 'md')
- positions_out: float32 [3, 32768], P(None, ('slab', 'md'))
- velocities_out: float32 [3, 32768], P(None, ('slab', 'md'))
- cell_moments: float32 [4, 16, 256], P(None, 'slab', 'md')
The draws below stay inside these ranges and needn't reach their ends.
Inputs may be any that keep to these rules, and one draw needn't show every extreme that they name: The 64 entries of one z position on one device name any owner at most 8 times in each column k and across k; the 2 owners of one cell differ. `neighbours`: entries index atoms of the same subdomain's block of 1024 atoms; an atom that lists itself is padding.
All inputs are finite; a program needn't handle non-finite values.
Results may differ from the reference program's by a relative error of at most 0.0003.
Values sent between devices are 32-bit elements; how exact they have to be, the bound alone decides.
A program may use at most 64 MiB of HBM per device.

```python
import math
import jax
import jax.numpy as jnp
import numpy as np
from jax import lax

CZ = 2
CX = 64
NY = 128
ATOMS = 1024
NBR = 64
TOP = 2
LB_STEPS = 4
MD_STEPS = 5
NZ = 16
NX = 256
ATOMS_ALL = 32768
MOST = 8
CAP = 16
SLOTS = 512
N_SLAB = 8
N_MD = 4
DEVICES = 32


def plant(values, own_key, smallest, top_value):
    longest = values.shape.index(max(values.shape))
    spots = []
    for shift in (0, 1):
        where = [jax.random.randint(jax.random.fold_in(own_key, axis), (), 0, length) for axis, length in enumerate(values.shape)]
        where[longest] = (where[longest] + shift) % values.shape[longest]
        spots.append(tuple(where))
    return values.at[spots[0]].set(smallest).at[spots[1]].set(top_value)


def block_scale(stream_key, shape, cuts, low, high):
    def one(position, shards_of):
        steps = jax.random.uniform(jax.random.fold_in(jax.random.fold_in(stream_key, 6), position), (shards_of,), jnp.float32, low / len(cuts), high / len(cuts))
        return jnp.repeat(jnp.exp(steps), shape[position] // shards_of).reshape((-1,) + (1,) * (len(shape) - position - 1))

    gain = one(*cuts[0])
    for cut in cuts[1:]:
        gain = gain * one(*cut)
    return gain


def deal_out(key, own, number, rows, count, top, bound, lean):
    sequence = jax.random.permutation(key, count)
    packed, common = load_shares(count, rows * top, bound, lean, True), load_shares(count, rows * top, bound, lean, False)
    places = jnp.arange(count)

    def named(lengths, turn):
        used = int((lengths > 0).sum())
        fixed = max(1, used // 4)
        moved = fixed + (places - fixed + turn * (used - fixed)) % max(1, count - fixed)
        return jnp.zeros((count,), jnp.int32).at[sequence[jnp.where(places < fixed, places, moved)]].set(jnp.asarray(lengths, jnp.int32))

    lengths = jnp.where(number % 4 == 0, named(packed, number // 4), named(common, number - number // 4 - 1))
    mixed = jax.random.permutation(jax.random.fold_in(own, 3), count)
    giver, taker = mixed[0:count // 2 * 2:2], mixed[1:count // 2 * 2:2]
    slack = jnp.minimum(lengths[giver] - 1, bound - lengths[taker]) // 2
    slack = jnp.where((giver == sequence[0]) | (taker == sequence[0]) | (lengths[taker] == 0), 0, jnp.maximum(slack, 0))
    moved = jax.random.randint(jax.random.fold_in(own, 4), (count // 2,), 0, 1 << 20) % (slack + 1)
    lengths = lengths.at[giver].add(-moved).at[taker].add(moved)
    items = jnp.searchsorted(jnp.cumsum(lengths), jnp.arange(rows * top), side="right").astype(jnp.int32)
    listing = items.reshape(top, rows).T
    listing = listing[jax.random.permutation(jax.random.fold_in(own, 1), rows)]
    turn = jax.random.randint(jax.random.fold_in(own, 2), (rows, 1), 0, top)
    return jnp.take_along_axis(listing, (jnp.arange(top)[None, :] + turn) % top, axis=1)


def load_shares(amount, total, reach, skew, full):
    loads = [(1 << 20) // math.isqrt(grade ** skew) + 1 for grade in range(1, amount + 1)]
    largest = reach if full else min(reach, max(-(-total // amount), total * loads[0] // sum(loads)))
    least = 1 if total - largest >= amount - 1 else 0
    counts, spare = [largest] + [least] * (amount - 1), total - largest - least * (amount - 1)
    while spare > 0:
        movable = [i for i in range(1, amount) if counts[i] < largest] or [i for i in range(1, amount) if counts[i] < reach]
        whole, budget = sum([loads[i] for i in movable]), spare
        for i in movable:
            more = min(reach - counts[i], max(1, budget * loads[i] // whole), spare)
            counts[i] = counts[i] + more
            spare = spare - more
    return np.array(counts)


def bell_draw(rng, dims, deviation, limit, cuts=(), kind=jnp.bfloat16):
    drawn = deviation * jax.random.normal(rng, dims, jnp.float32)
    if cuts:
        drawn = drawn * block_scale(rng, dims, cuts, -0.22, 0.18)
    return jnp.clip(drawn, -limit, limit).astype(kind)


def setup_inputs(seed: int = 0) -> dict:
    keys = jax.random.split(jax.random.key(seed), 8)
    populations = jnp.clip(0.02 + 0.08 * jax.random.uniform(keys[0], (19, NZ, NX, NY), jnp.float32) ** block_scale(keys[0], (19, NZ, NX, NY), ((1, 8), (2, 4)), -0.2, 0.2), 0.02, 0.1)
    relax = jnp.clip(jnp.exp(math.log(1.8) - 0.8109302 * jax.random.uniform(keys[1], (NZ, NX, NY), jnp.float32) ** block_scale(keys[1], (NZ, NX, NY), ((0, 8), (1, 4)), -0.2, 0.2)), 0.8, 1.8)
    owners_keys = jax.random.split(jax.random.fold_in(keys[2], 1), NZ * NX // CX)
    owners_turns = jax.random.permutation(jax.random.fold_in(keys[2], 3), NZ * NX // CX)
    owners = jax.vmap(lambda own, number: deal_out(jax.random.fold_in(keys[2], 2), own, number, CX, DEVICES, TOP, MOST, 2))(owners_keys, owners_turns).reshape((NZ, NX, TOP))
    positions = jnp.clip(3.0 * jax.random.uniform(keys[3], (3, ATOMS_ALL), jnp.float32) ** block_scale(keys[3], (3, ATOMS_ALL), ((1, 32),), -0.2, 0.2), 0.0, 3.0)
    velocities = bell_draw(keys[4], (3, ATOMS_ALL), 1.0, 5.0, ((1, 32),), jnp.float32)
    neighbours = plant(jax.random.randint(keys[5], (ATOMS_ALL, NBR), 0, ATOMS), jax.random.fold_in(keys[5], 1), 0, ATOMS - 1).astype(jnp.int32)
    atom_slots = plant(jax.random.randint(keys[6], (ATOMS_ALL,), 0, SLOTS), jax.random.fold_in(keys[6], 1), 0, SLOTS - 1).astype(jnp.int32)
    return dict(populations=populations, relax=relax, owners=owners, positions=positions, velocities=velocities, neighbours=neighbours, atom_slots=atom_slots)


lattice_dirs = [(0, 0, 0), (1, 0, 0), (-1, 0, 0), (0, 1, 0), (0, -1, 0), (0, 0, 1), (0, 0, -1),
                (1, 1, 0), (-1, -1, 0), (1, -1, 0), (-1, 1, 0), (1, 0, 1), (-1, 0, -1), (1, 0, -1),
                (-1, 0, 1), (0, 1, 1), (0, -1, -1), (0, 1, -1), (0, -1, 1)]
lattice_weights = [1.0 / 3.0] + [1.0 / 18.0] * 6 + [1.0 / 36.0] * 12
velocity_scale = 10.0
pair_strength = 0.5
friction = 2.0
time_step = 0.1


def velocity(f, density):
    comps = []
    for axis_id in range(3):
        total = jnp.zeros_like(density)
        for index, direction in enumerate(lattice_dirs):
            if direction[axis_id] != 0:
                total = total + direction[axis_id] * f[index]
        comps.append(total / density)
    return comps


def collide(f, relax):
    density = jnp.sum(f, axis=0)
    vel_x, vel_y, vel_z = velocity(f, density)
    usq = vel_x * vel_x + vel_y * vel_y + vel_z * vel_z
    result = []
    for index, direction in enumerate(lattice_dirs):
        along = direction[0] * vel_x + direction[1] * vel_y + direction[2] * vel_z
        equil = lattice_weights[index] * density * (1.0 + 3.0 * along + 4.5 * along * along - 1.5 * usq)
        result.append(f[index] - relax * (f[index] - equil))
    return result


def md_run(pos, vel, nbr, slots, recv):
    target = recv[slots]
    goal = target[:, :3].T
    dens = target[:, 3]
    for step in range(MD_STEPS):
        gap = pos[:, nbr] - pos[:, :, None]
        weight = jnp.exp(-0.5 * jnp.sum(gap * gap, axis=0))
        force = pair_strength * jnp.sum(gap * weight[None], axis=2) + friction * dens[None, :] * (goal - vel)
        vel = vel + time_step * force
        pos = pos + time_step * vel
    data = jnp.concatenate([vel, jnp.sum(vel * vel, axis=0, keepdims=True)], axis=0).T
    sums = jax.ops.segment_sum(data, slots, num_segments=recv.shape[0])
    count = jax.ops.segment_sum(jnp.ones(slots.shape, jnp.float32), slots, num_segments=recv.shape[0])
    return pos, vel, sums / jnp.maximum(count, 1.0)[:, None]


def reference(populations, relax, owners, positions, velocities, neighbours, atom_slots):
    f = populations
    for step in range(LB_STEPS):
        post = collide(f, relax)
        f = jnp.stack([jnp.roll(post[i], (c[2], c[0], c[1]), axis=(0, 1, 2)) for i, c in enumerate(lattice_dirs)])
    density = jnp.sum(f, axis=0)
    vel_x, vel_y, vel_z = velocity(f, density)
    targets = jnp.stack([jnp.mean(velocity_scale * vel_x, axis=2), jnp.mean(velocity_scale * vel_y, axis=2),
                         jnp.mean(velocity_scale * vel_z, axis=2), jnp.mean(density, axis=2)])
    devices = N_SLAB * N_MD
    entries = CZ * CX * TOP
    tgt_dev = targets.reshape(4, N_SLAB, CZ, N_MD, CX).transpose(1, 3, 0, 2, 4).reshape(devices, 4, CZ * CX)
    vals = jnp.repeat(tgt_dev, TOP, axis=2).transpose(0, 2, 1)
    own = owners.reshape(N_SLAB, CZ, N_MD, CX, TOP).transpose(0, 2, 1, 3, 4).reshape(devices, entries)
    labels = jnp.arange(devices, dtype=jnp.int32)

    def ranks_of(row):
        onehot = (row[:, None] == labels[None, :]).astype(jnp.int32)
        before = jnp.cumsum(onehot, axis=0) - onehot
        return jnp.sum(before * onehot, axis=1).astype(jnp.int32)

    rank = lax.map(ranks_of, own)
    slot = (labels[:, None] * CAP + rank).astype(jnp.int32)
    pos_dev = positions.reshape(3, devices, ATOMS).transpose(1, 0, 2)
    vel_dev = velocities.reshape(3, devices, ATOMS).transpose(1, 0, 2)
    nbr_dev = neighbours.reshape(devices, ATOMS, NBR)
    slot_dev = atom_slots.reshape(devices, ATOMS)

    def per_owner(back, inputs):
        owner_id, pos, vel, nbr, slots = inputs
        hit = own == owner_id
        where_to = jnp.where(hit, slot, SLOTS).astype(jnp.int32)
        recv = jnp.zeros((SLOTS, 4), jnp.float32).at[where_to].set(vals, mode="drop")
        pos, vel, moms = md_run(pos, vel, nbr, slots, recv)
        back = back + jnp.where(hit[:, :, None], moms[slot], 0.0)
        return back, (pos, vel)

    back, (pos_out, vel_out) = lax.scan(per_owner, jnp.zeros((devices, entries, 4), jnp.float32),
                                        (labels, pos_dev, vel_dev, nbr_dev, slot_dev))
    summed = back.reshape(devices, CZ * CX, TOP, 4).sum(axis=2).transpose(0, 2, 1)
    cell_moments = summed.reshape(N_SLAB, N_MD, 4, CZ, CX).transpose(2, 0, 3, 1, 4).reshape(4, NZ, NX)
    positions_out = pos_out.transpose(1, 0, 2).reshape(3, ATOMS_ALL)
    velocities_out = vel_out.transpose(1, 0, 2).reshape(3, ATOMS_ALL)
    return f, positions_out, velocities_out, cell_moments
```

```python
import functools

import jax
import jax.numpy as jnp
from jax import lax
from jax.experimental import pallas as pl
from jax.experimental.pallas import tpu as pltpu
from jax.sharding import PartitionSpec as P

LB_STEPS = 4
MD_STEPS = 5

ORDER = [13, 1, 7, 9, 11, 5, 15, 18, 14, 2, 8, 10, 12, 6, 16, 17, 0, 3, 4]
lattice_dirs = [
    (0, 0, 0),
    (1, 0, 0),
    (-1, 0, 0),
    (0, 1, 0),
    (0, -1, 0),
    (0, 0, 1),
    (0, 0, -1),
    (1, 1, 0),
    (-1, -1, 0),
    (1, -1, 0),
    (-1, 1, 0),
    (1, 0, 1),
    (-1, 0, -1),
    (1, 0, -1),
    (-1, 0, 1),
    (0, 1, 1),
    (0, -1, -1),
    (0, 1, -1),
    (0, -1, 1),
]
DIRS = [lattice_dirs[i] for i in ORDER]
velocity_scale = 10.0
pair_strength = 0.5
friction = 2.0
time_step = 0.1
highest = lax.Precision.HIGHEST
MESH = pl.DeviceIdType.MESH


def total_of(terms):
    terms = list(terms)
    while len(terms) > 1:
        terms = [a + b for a, b in zip(terms[::2], terms[1::2])] + (
            [terms[-1]] if len(terms) % 2 else []
        )
    return terms[0]


def fields(f):
    density = total_of(f)
    inverse = 1.0 / density
    vel = []
    for axis in range(3):
        plus = total_of(f[p] for p in range(19) if DIRS[p][axis] == 1)
        minus = total_of(f[p] for p in range(19) if DIRS[p][axis] == -1)
        vel.append((plus - minus) * inverse)
    return density, vel


def collided(f, relax):
    density, (vx, vy, vz) = fields(f)
    base = 1.0 - 1.5 * (vx * vx + vy * vy + vz * vz)
    keep = 1.0 - relax
    scale = relax * density
    result = [None] * 19
    for p, c in enumerate(DIRS):
        if result[p] is not None:
            continue
        size = sum(abs(e) for e in c)
        if size == 0:
            result[p] = keep * f[p] + (scale * (1.0 / 3.0)) * base
            continue
        along = total_of(v if e == 1 else -v for e, v in zip(c, (vx, vy, vz)) if e)
        weight = scale * (1.0 / 18.0 if size == 1 else 1.0 / 36.0)
        even = weight * (base + 4.5 * (along * along))
        odd = weight * (3.0 * along)
        q = DIRS.index(tuple(-e for e in c))
        result[p] = keep * f[p] + (even + odd)
        result[q] = keep * f[q] + (even - odd)
    return result


def lattice_kernel(
    n_slab, n_md, f_ref, relax_ref, out_ref, tgt_ref, post, rows_out, rows_in, mean_ref, send, recv
):
    cz, cx, ny = relax_ref.shape
    slab, md = lax.axis_index("slab"), lax.axis_index("md")
    above, below = lax.rem(slab + 1, n_slab), lax.rem(slab + n_slab - 1, n_slab)
    right, left = lax.rem(md + 1, n_md), lax.rem(md + n_md - 1, n_md)
    barrier = pltpu.get_barrier_semaphore()
    peers = [
        (above, md),
        (below, md),
        (slab, right),
        (slab, left),
        (above, right),
        (below, right),
        (above, left),
        (below, left),
    ]
    for peer in peers:
        pl.semaphore_signal(barrier, inc=1, device_id=peer, device_id_type=MESH)

    def load(step, z, x0):
        if step == 0:
            return [f_ref[ORDER[p], z, pl.ds(x0, 8), :] for p in range(19)]
        return [
            post[step - 1, p, z + 1 - c[2], pl.ds(x0 + (8 - c[0]), 8), :]
            for p, c in enumerate(DIRS)
        ]

    def plane(step, z):
        def block(b, carry):
            x0 = pl.multiple_of(b * 8, 8)
            done = collided(load(step, z, x0), relax_ref[z, pl.ds(x0, 8), :])
            for p, c in enumerate(DIRS):
                value = done[p] if c[1] == 0 else pltpu.roll(done[p], c[1] % ny, axis=1)
                post[step, p, z + 1, pl.ds(x0 + 8, 8), :] = value
            return carry

        lax.fori_loop(0, cx // 8, block, 0, unroll=2)

    copies = []
    for step in range(LB_STEPS):

        def copy(slot, src, dst, peer):
            made = pltpu.make_async_remote_copy(
                src_ref=src,
                dst_ref=dst,
                send_sem=send.at[step, slot],
                recv_sem=recv.at[step, slot],
                device_id=peer,
                device_id_type=MESH,
            )
            made.start()
            copies.append(made)
            return made

        now = []
        own = pl.ds(8, cx)
        plane(step, cz - 1)
        if step == 0:
            pl.semaphore_wait(barrier, len(peers))
        now.append(
            copy(
                0,
                post.at[step, pl.ds(4, 5), cz, own, :],
                post.at[step, pl.ds(4, 5), 0, own, :],
                (above, md),
            )
        )
        for z in range(cz - 1):
            plane(step, z)
        for slot, first, count in ((1, 12, 4), (2, 0, 1)):
            now.append(
                copy(
                    slot,
                    post.at[step, pl.ds(first, count), 1, own, :],
                    post.at[step, pl.ds(first, count), cz + 1, own, :],
                    (below, md),
                )
            )
        for side, first, row in ((0, 0, 7 + cx), (1, 8, 8)):
            for j in range(5):
                for z in range(cz):
                    rows_out[step, side, j * cz + z, :] = post[step, first + j, z + 1, row, :]
        for k, (p, z, row) in enumerate(
            ((4, cz, 7 + cx), (0, 1, 7 + cx), (8, cz, 8), (12, 1, 8))
        ):
            rows_out[step, 2 + k, 0, :] = post[step, p, z, row, :]
        for k in range(6):
            height = rows_out.shape[2] if k < 2 else 8
            now.append(
                copy(
                    3 + k,
                    rows_out.at[step, k, pl.ds(0, height), :],
                    rows_in.at[step, k, pl.ds(0, height), :],
                    peers[2 + k],
                )
            )
        for made in now:
            made.wait_recv()
        for side, first, row in ((0, 0, 7), (1, 8, 8 + cx)):
            for j in range(5):
                for z in range(cz):
                    post[step, first + j, z + 1, row, :] = rows_in[step, side, j * cz + z, :]
        for k, (p, z, row) in enumerate(
            ((4, 0, 7), (0, cz + 1, 7), (8, 0, 8 + cx), (12, cz + 1, 8 + cx))
        ):
            post[step, p, z, row, :] = rows_in[step, 2 + k, 0, :]

    for z in range(cz):

        def last(b, carry, z=z):
            x0 = pl.multiple_of(b * 8, 8)
            f = load(LB_STEPS, z, x0)
            for p in range(19):
                out_ref[ORDER[p], z, pl.ds(x0, 8), :] = f[p]
            density, vel = fields(f)
            for c, value in enumerate((*vel, density)):
                mean_ref[c, pl.ds(x0 + z * cx, 8), :] = value
            return carry

        lax.fori_loop(0, cx // 8, last, 0, unroll=2)
    for c in range(4):
        scale = (velocity_scale if c < 3 else 1.0) / ny
        tgt_ref[pl.ds(c, 1), :] = jnp.sum(mean_ref[c].T, axis=0, keepdims=True) * scale
    for made in copies:
        made.wait_send()


def lattice(populations, relax, n_slab, n_md):
    cz, cx, ny = relax.shape
    rows = -(-5 * cz // 8) * 8
    vmem = pl.BlockSpec(memory_space=pltpu.VMEM)
    return pl.pallas_call(
        functools.partial(lattice_kernel, n_slab, n_md),
        out_shape=(
            jax.ShapeDtypeStruct(populations.shape, jnp.float32),
            jax.ShapeDtypeStruct((4, cz * cx), jnp.float32),
        ),
        in_specs=[vmem, vmem],
        out_specs=(vmem, vmem),
        scratch_shapes=[
            pltpu.VMEM((LB_STEPS, 19, cz + 2, cx + 16, ny), jnp.float32),
            pltpu.VMEM((LB_STEPS, 6, rows, ny), jnp.float32),
            pltpu.VMEM((LB_STEPS, 6, rows, ny), jnp.float32),
            pltpu.VMEM((4, cz * cx, ny), jnp.float32),
            pltpu.SemaphoreType.DMA((LB_STEPS, 9)),
            pltpu.SemaphoreType.DMA((LB_STEPS, 9)),
        ],
        compiler_params=pltpu.CompilerParams(
            collective_id=0, has_side_effects=True, vmem_limit_bytes=32 * 1024 * 1024
        ),
        name="lattice",
    )(populations, relax)


def lane_gather(table, index):
    return jnp.take_along_axis(table, index, axis=1, mode="promise_in_bounds")


def particle_kernel(
    pos_ref, vel_ref, nbr_ref, slots_ref, recv_ref, pos_out, vel_out, mom_ref, lists, at, pull, data, hits
):
    atoms, entries = nbr_ref.shape
    groups = atoms // 128
    slot_count = recv_ref.shape[1]
    for g in range(groups):
        here = pl.ds(g * 128, 128)
        lists[g] = nbr_ref[here, :].T
        for c in range(3):
            at[c, pl.ds(g, 1), :] = pos_ref[pl.ds(c, 1), here]
            at[3 + c, pl.ds(g, 1), :] = vel_ref[pl.ds(c, 1), here]
        label = lax.broadcasted_iota(jnp.int32, (slot_count, 128), 0)
        same = label == slots_ref[pl.ds(g, 1), :]
        hits[:, here] = jnp.where(same, 1.0, 0.0).astype(jnp.bfloat16)
    slots = slots_ref[...]
    lane, row = slots & 127, slots >> 7
    goal = []
    for c in range(4):
        value = jnp.zeros((groups, 128), jnp.float32)
        for h in range(slot_count // 128):
            table = jnp.broadcast_to(recv_ref[pl.ds(c, 1), pl.ds(h * 128, 128)], (groups, 128))
            value = jnp.where(row == h, lane_gather(table, lane), value)
        goal.append(value)
    rate = friction * goal[3]

    def one_step(step, carry):
        def one_group(g, inner):
            own = [jnp.broadcast_to(at[c, pl.ds(g, 1), :], (8, 128)) for c in range(3)]
            sums = [jnp.zeros((8, 128), jnp.float32)] * 3
            for k in range(0, entries, 8):
                index = lists[g, pl.ds(k, 8), :]
                lane, row = index & 127, index >> 7
                found = [None] * 3
                for h in range(groups):
                    pick = row == h
                    for c in range(3):
                        table = jnp.broadcast_to(at[c, pl.ds(h, 1), :], (8, 128))
                        value = lane_gather(table, lane)
                        found[c] = value if h == 0 else jnp.where(pick, value, found[c])
                gap = [found[c] - own[c] for c in range(3)]
                weight = jnp.exp(-0.5 * (gap[0] * gap[0] + gap[1] * gap[1] + gap[2] * gap[2]))
                sums = [sums[c] + gap[c] * weight for c in range(3)]
            for c in range(3):
                pull[c, pl.ds(g, 1), :] = jnp.sum(sums[c], axis=0, keepdims=True)
            return inner

        lax.fori_loop(0, groups, one_group, 0)
        for c in range(3):
            vel = at[3 + c]
            force = pair_strength * pull[c] + rate * (goal[c] - vel)
            vel = vel + time_step * force
            at[3 + c] = vel
            at[c] = at[c] + time_step * vel
        return carry

    lax.fori_loop(0, MD_STEPS, one_step, 0)
    at[6] = at[3] * at[3] + at[4] * at[4] + at[5] * at[5]
    data[...] = jnp.ones(data.shape, jnp.float32)
    for c in range(4):
        rest = at[3 + c]
        for part in range(3):
            piece = rest.astype(jnp.bfloat16).astype(jnp.float32)
            rest = rest - piece
            for g in range(groups):
                data[pl.ds(part * 4 + c, 1), pl.ds(g * 128, 128)] = piece[g : g + 1, :]
    for g in range(groups):
        here = pl.ds(g * 128, 128)
        for c in range(3):
            pos_out[pl.ds(c, 1), here] = at[c, pl.ds(g, 1), :]
            vel_out[pl.ds(c, 1), here] = at[3 + c, pl.ds(g, 1), :]
    sums = lax.dot_general(
        data[...].astype(jnp.bfloat16),
        hits[...],
        (((1,), (1,)), ((), ())),
        preferred_element_type=jnp.float32,
    )
    mom_ref[...] = (sums[0:4] + sums[4:8] + sums[8:12]) / jnp.maximum(sums[12:13], 1.0)


def particles(pos, vel, nbr, slots, recv):
    atoms, entries = nbr.shape
    slot_count = recv.shape[1]
    groups = atoms // 128
    vmem = pl.BlockSpec(memory_space=pltpu.VMEM)
    return pl.pallas_call(
        particle_kernel,
        out_shape=(
            jax.ShapeDtypeStruct(pos.shape, jnp.float32),
            jax.ShapeDtypeStruct(vel.shape, jnp.float32),
            jax.ShapeDtypeStruct((4, slot_count), jnp.float32),
        ),
        in_specs=[vmem] * 5,
        out_specs=(vmem,) * 3,
        scratch_shapes=[
            pltpu.VMEM((groups, entries, 128), jnp.int32),
            pltpu.VMEM((7, groups, 128), jnp.float32),
            pltpu.VMEM((3, groups, 128), jnp.float32),
            pltpu.VMEM((16, atoms), jnp.float32),
            pltpu.VMEM((slot_count, atoms), jnp.bfloat16),
        ],
        name="particles",
    )(pos, vel, nbr, slots.reshape(groups, 128), recv)


def on_device(populations, relax, owners, positions, velocities, neighbours, atom_slots):
    cz_len, cx_len, _ = relax.shape
    n_slab = lax.axis_size("slab")
    n_md = lax.axis_size("md")
    f, targets = lattice(populations, relax, n_slab, n_md)
    top = owners.shape[2]
    devices = n_slab * n_md
    most = max(2, 2 * cx_len * top // devices)
    cap = cz_len * most
    own = owners.reshape(-1)
    onehot = (own[:, None] == jnp.arange(devices, dtype=jnp.int32)[None, :]).astype(jnp.int32)
    rank = jnp.sum((jnp.cumsum(onehot, axis=0) - onehot) * onehot, axis=1)
    dest = own * cap + rank
    placed = (dest[:, None] == jnp.arange(devices * cap, dtype=jnp.int32)[None, :]).astype(
        jnp.float32
    )
    vals = jnp.repeat(targets, top, axis=1)
    outgoing = jnp.dot(vals, placed, precision=highest, preferred_element_type=jnp.float32)
    arrived = lax.all_to_all(
        outgoing.reshape(4, devices, cap), ("slab", "md"), split_axis=1, concat_axis=1, tiled=True
    )
    arrived = arrived.reshape(4, devices * cap)
    pos_out, vel_out, moms = particles(positions, velocities, neighbours, atom_slots, arrived)
    returned = lax.all_to_all(
        moms.reshape(4, devices, cap), ("slab", "md"), split_axis=1, concat_axis=1, tiled=True
    )
    returned = returned.reshape(4, devices * cap)
    picked = jnp.dot(returned, placed.T, precision=highest, preferred_element_type=jnp.float32)
    cell_moments = jnp.sum(picked.reshape(4, cz_len * cx_len, top), axis=2).reshape(
        4, cz_len, cx_len
    )
    return (f, pos_out, vel_out, cell_moments)


def solution(mesh):
    return jax.shard_map(
        on_device,
        mesh=mesh,
        in_specs=(
            P(None, "slab", "md", None),
            P("slab", "md", None),
            P("slab", "md", None),
            P(None, ("slab", "md")),
            P(None, ("slab", "md")),
            P(("slab", "md"), None),
            P(("slab", "md")),
        ),
        out_specs=(
            P(None, "slab", "md", None),
            P(None, ("slab", "md")),
            P(None, ("slab", "md")),
            P(None, "slab", "md"),
        ),
        check_vma=False,
    )
```

```python
import functools

import jax
import jax.numpy as jnp
from jax import lax
from jax.experimental import pallas as pl
from jax.experimental.pallas import tpu as pltpu
from jax.sharding import PartitionSpec as P

LB_STEPS = 4
MD_STEPS = 5

ORDER = [13, 1, 7, 9, 11, 5, 15, 18, 14, 2, 8, 10, 12, 6, 16, 17, 0, 3, 4]
lattice_dirs = [
    (0, 0, 0),
    (1, 0, 0),
    (-1, 0, 0),
    (0, 1, 0),
    (0, -1, 0),
    (0, 0, 1),
    (0, 0, -1),
    (1, 1, 0),
    (-1, -1, 0),
    (1, -1, 0),
    (-1, 1, 0),
    (1, 0, 1),
    (-1, 0, -1),
    (1, 0, -1),
    (-1, 0, 1),
    (0, 1, 1),
    (0, -1, -1),
    (0, 1, -1),
    (0, -1, 1),
]
DIRS = [lattice_dirs[i] for i in ORDER]
velocity_scale = 10.0
pair_strength = 0.5
friction = 2.0
time_step = 0.1
MESH = pl.DeviceIdType.MESH


def total_of(terms):
    terms = list(terms)
    while len(terms) > 1:
        terms = [a + b for a, b in zip(terms[::2], terms[1::2])] + (
            [terms[-1]] if len(terms) % 2 else []
        )
    return terms[0]


def fields(f):
    density = total_of(f)
    inverse = 1.0 / density
    vel = []
    for axis in range(3):
        plus = total_of(f[p] for p in range(19) if DIRS[p][axis] == 1)
        minus = total_of(f[p] for p in range(19) if DIRS[p][axis] == -1)
        vel.append((plus - minus) * inverse)
    return density, vel


def collided(f, relax):
    density, (vx, vy, vz) = fields(f)
    base = 1.0 - 1.5 * (vx * vx + vy * vy + vz * vz)
    keep = 1.0 - relax
    scale = relax * density
    result = [None] * 19
    for p, c in enumerate(DIRS):
        if result[p] is not None:
            continue
        size = sum(abs(e) for e in c)
        if size == 0:
            result[p] = keep * f[p] + (scale * (1.0 / 3.0)) * base
            continue
        along = total_of(v if e == 1 else -v for e, v in zip(c, (vx, vy, vz)) if e)
        weight = scale * (1.0 / 18.0 if size == 1 else 1.0 / 36.0)
        even = weight * (base + 4.5 * (along * along))
        odd = weight * (3.0 * along)
        q = DIRS.index(tuple(-e for e in c))
        result[p] = keep * f[p] + (even + odd)
        result[q] = keep * f[q] + (even - odd)
    return result


def lane_gather(table, index):
    return jnp.take_along_axis(table, index, axis=1, mode="promise_in_bounds")


def thirds(value):
    parts = []
    for _ in range(3):
        piece = value.astype(jnp.bfloat16).astype(jnp.float32)
        parts.append(piece)
        value = value - piece
    return parts


def by_hits(data, hits, dims):
    return lax.dot_general(
        data.astype(jnp.bfloat16), hits, (dims, ((), ())), preferred_element_type=jnp.float32
    )


def coupled_kernel(
    n_slab,
    n_md,
    f_ref,
    relax_ref,
    own_ref,
    pos_ref,
    vel_ref,
    nbr_ref,
    slots_ref,
    out_ref,
    pos_out,
    vel_out,
    cell_out,
    post,
    rows_out,
    rows_in,
    mean_ref,
    at,
    pull,
    data,
    hits,
    placed,
    tgt,
    table,
    blocks_out,
    blocks_in,
    send,
    recv,
    swap_send,
    swap_recv,
):
    cz, cx, ny = relax_ref.shape
    top_z = cz - 1
    cells = cz * cx
    entries, atoms = nbr_ref.shape
    groups = atoms // 128
    slot_count = hits.shape[0]
    devices = n_slab * n_md
    cap = slot_count // devices
    slab, md = lax.axis_index("slab"), lax.axis_index("md")
    me = slab * n_md + md
    above, below = lax.rem(slab + 1, n_slab), lax.rem(slab + n_slab - 1, n_slab)
    right, left = lax.rem(md + 1, n_md), lax.rem(md + n_md - 1, n_md)
    barrier = pltpu.get_barrier_semaphore()

    def coords(device):
        return (lax.div(device, n_md), lax.rem(device, n_md))

    def greet(k, carry):
        peer = coords(lax.rem(me + k, devices))
        pl.semaphore_signal(barrier, inc=1, device_id=peer, device_id_type=MESH)
        return carry

    lax.fori_loop(1, devices, greet, 0)

    def load(step, z, x0):
        if step == 0:
            return [f_ref[ORDER[p], z, pl.ds(x0, 8), :] for p in range(19)]
        return [
            post[step - 1, p, z + 1 - c[2], pl.ds(x0 + (8 - c[0]), 8), :]
            for p, c in enumerate(DIRS)
        ]

    def plane(step, z):
        def block(b, carry):
            x0 = pl.multiple_of(b * 8, 8)
            done = collided(load(step, z, x0), relax_ref[z, pl.ds(x0, 8), :])
            for p, c in enumerate(DIRS):
                value = done[p] if c[1] == 0 else pltpu.roll(done[p], c[1] % ny, axis=1)
                post[step, p, z + 1, pl.ds(x0 + 8, 8), :] = value
            return carry

        lax.fori_loop(0, cx // 8, block, 0, unroll=2)
        for side, first, row in ((0, 0, 7 + cx), (1, 8, 8)):
            for j in range(5):
                rows_out[step, z, side, j, :] = post[step, first + j, z + 1, row, :]

    copies = []

    def copy(step, slot, src, dst, peer):
        made = pltpu.make_async_remote_copy(
            src_ref=src,
            dst_ref=dst,
            send_sem=send.at[step, slot],
            recv_sem=recv.at[step, slot],
            device_id=peer,
            device_id_type=MESH,
        )
        made.start()
        copies.append(made)
        return made

    own = pl.ds(8, cx)

    def send_rows(step, z):
        return [
            copy(
                step,
                7 + 2 * z + side,
                rows_out.at[step, z, side],
                rows_in.at[step, z + 1, side],
                (slab, (right, left)[side]),
            )
            for side in range(2)
        ]

    def send_z(step, rising):
        z, slot, peer = (top_z, 0, above) if rising else (0, cz + 1, below)
        base = 0 if rising else 3
        made = [
            copy(
                step,
                base + 1 + side,
                rows_out.at[step, z, side],
                rows_in.at[step, slot, side],
                (peer, (right, left)[side]),
            )
            for side in range(2)
        ]
        spans = ((4, 5, 0),) if rising else ((12, 4, 3), (0, 1, 6))
        for first, count, sem in spans:
            made.append(
                copy(
                    step,
                    sem,
                    post.at[step, pl.ds(first, count), z + 1, own, :],
                    post.at[step, pl.ds(first, count), slot, own, :],
                    (peer, md),
                )
            )
        return made

    def arrive(made):
        for one in made:
            one.wait_recv()

    def put_rows(step):
        for z in range(cz):
            for side, first, row in ((0, 0, 7), (1, 8, 8 + cx)):
                for j in range(5):
                    post[step, first + j, z + 1, row, :] = rows_in[step, z + 1, side, j, :]

    def put_corners(step, rising):
        slot = 0 if rising else cz + 1
        for side, row in ((0, 7), (1, 8 + cx)):
            j = (4, 0)[side] if rising else (0, 4)[side]
            post[step, 8 * side + j, slot, row, :] = rows_in[step, slot, side, j, :]

    def pair_forces():
        def one_group(g, inner):
            mine = [jnp.broadcast_to(at[c, pl.ds(g, 1), :], (8, 128)) for c in range(3)]
            sums = [jnp.zeros((8, 128), jnp.float32)] * 3
            for k in range(0, entries, 8):
                index = nbr_ref[pl.ds(k, 8), pl.ds(pl.multiple_of(g * 128, 128), 128)]
                lane, row = index & 127, index >> 7
                found = [None] * 3
                for h in range(groups):
                    pick = row == h
                    for c in range(3):
                        line = jnp.broadcast_to(at[c, pl.ds(h, 1), :], (8, 128))
                        value = lane_gather(line, lane)
                        found[c] = value if h == 0 else jnp.where(pick, value, found[c])
                gap = [found[c] - mine[c] for c in range(3)]
                weight = jnp.exp(-0.5 * (gap[0] * gap[0] + gap[1] * gap[1] + gap[2] * gap[2]))
                sums = [sums[c] + gap[c] * weight for c in range(3)]
            for c in range(3):
                pull[c, pl.ds(g, 1), :] = jnp.sum(sums[c], axis=0, keepdims=True)
            return inner

        lax.fori_loop(0, groups, one_group, 0)

    def prepare_particles():
        for g in range(groups):
            here = pl.ds(g * 128, 128)
            for c in range(3):
                at[c, pl.ds(g, 1), :] = pos_ref[pl.ds(c, 1), here]
                at[3 + c, pl.ds(g, 1), :] = vel_ref[pl.ds(c, 1), here]
        pair_forces()

    def prepare_hits():
        data[...] = jnp.ones(data.shape, jnp.float32)
        tgt[...] = jnp.zeros(tgt.shape, jnp.float32)
        table[...] = jnp.zeros(table.shape, jnp.float32)
        for g in range(groups):
            label = lax.broadcasted_iota(jnp.int32, (slot_count, 128), 0)
            same = label == slots_ref[pl.ds(g, 1), :]
            hits[:, pl.ds(g * 128, 128)] = jnp.where(same, 1.0, 0.0).astype(jnp.bfloat16)

    def prepare_routes():
        top = own_ref.shape[0]
        label = lax.broadcasted_iota(jnp.int32, (devices, cells), 0)
        owned = [jnp.where(label == own_ref[pl.ds(k, 1), :], 1.0, 0.0) for k in range(top)]
        earlier = lax.broadcasted_iota(jnp.int32, (cells, cells), 0) < lax.broadcasted_iota(
            jnp.int32, (cells, cells), 1
        )
        before = by_hits(
            total_of(owned), jnp.where(earlier, 1.0, 0.0).astype(jnp.bfloat16), ((1,), (0,))
        )
        start = (label * cap).astype(jnp.float32)
        place = lax.broadcasted_iota(jnp.int32, (slot_count, cells), 0).astype(jnp.float32)
        filled = jnp.zeros((slot_count, cells), jnp.float32)
        for k in range(top):
            spot = jnp.sum((before + start) * owned[k], axis=0, keepdims=True)
            filled = filled + jnp.where(place == spot, 1.0, 0.0)
            before = before + owned[k]
        placed[...] = filled.astype(jnp.bfloat16)

    def swap(turn, values):
        per = 128 // cap
        for d in range(devices):
            chunk = values[:, d // per * 128 : (d // per + 1) * 128]
            shift = (128 - d % per * cap) % 128
            blocks_out[turn, d] = chunk if shift == 0 else pltpu.roll(chunk, shift, axis=1)

        def trade(k):
            to = lax.rem(me + k, devices)
            return pltpu.make_async_remote_copy(
                src_ref=blocks_out.at[turn, to],
                dst_ref=blocks_in.at[turn, me],
                send_sem=swap_send.at[turn, k],
                recv_sem=swap_recv.at[turn, k],
                device_id=coords(to),
                device_id_type=MESH,
            )

        def begin(k, carry):
            trade(k).start()
            return carry

        def landed(k, carry):
            origin = lax.rem(me + devices - k, devices)
            pltpu.make_async_remote_copy(
                src_ref=blocks_out.at[turn, origin],
                dst_ref=blocks_in.at[turn, origin],
                send_sem=swap_send.at[turn, k],
                recv_sem=swap_recv.at[turn, k],
                device_id=coords(origin),
                device_id_type=MESH,
            ).wait_recv()
            return carry

        def sent(k, carry):
            trade(k).wait_send()
            return carry

        lax.fori_loop(1, devices, begin, 0)
        blocks_in[turn, me] = blocks_out[turn, me]
        lax.fori_loop(1, devices, landed, 0)
        zone = lax.broadcasted_iota(jnp.int32, (4, 128), 1) // cap
        lines = []
        for h in range(slot_count // 128):
            line = jnp.zeros((4, 128), jnp.float32)
            for j in range(per):
                value = blocks_in[turn, h * per + j]
                if j:
                    value = pltpu.roll(value, j * cap, axis=1)
                line = jnp.where(zone == j, value, line)
            lines.append(line)
        return lines, lambda: lax.fori_loop(1, devices, sent, 0)

    last = {}
    plane(0, 0)
    for z in range(1, top_z):
        plane(0, z)
    pl.semaphore_wait(barrier, devices - 1)
    rows = []
    for z in range(top_z):
        rows += send_rows(0, z)
    last[False] = send_z(0, False)
    plane(0, top_z)
    rows += send_rows(0, top_z)
    last[True] = send_z(0, True)
    prepare_particles()
    for step in range(1, LB_STEPS):
        arrive(rows)
        put_rows(step - 1)
        rows, coming = [], {}
        for rising in ((False, True), (True, False))[(step + 1) % 2]:
            arrive(last[rising])
            put_corners(step - 1, rising)
            levels = range(top_z) if rising else [top_z]
            for z in levels:
                plane(step, z)
                rows += send_rows(step, z)
            coming[not rising] = send_z(step, not rising)
        last = coming
        if step == 1:
            prepare_hits()
        if step == 2:
            prepare_routes()
    arrive(rows)
    put_rows(LB_STEPS - 1)
    for rising in ((False, True), (True, False))[(LB_STEPS + 1) % 2]:
        arrive(last[rising])
        put_corners(LB_STEPS - 1, rising)
        for z in range(top_z) if rising else [top_z]:

            def finish(b, carry, z=z):
                x0 = pl.multiple_of(b * 8, 8)
                f = load(LB_STEPS, z, x0)
                for p in range(19):
                    out_ref[ORDER[p], z, pl.ds(x0, 8), :] = f[p]
                density, vel = fields(f)
                for c, value in enumerate((*vel, density)):
                    mean_ref[c, pl.ds(x0 + z * cx, 8), :] = value
                return carry

            lax.fori_loop(0, cx // 8, finish, 0, unroll=2)
    for c in range(4):
        scale = (velocity_scale if c < 3 else 1.0) / ny
        mean = jnp.sum(mean_ref[c].T, axis=0, keepdims=True) * scale
        for part, piece in enumerate(thirds(mean)):
            tgt[pl.ds(part * 4 + c, 1), :] = piece
    sums = by_hits(tgt[...], placed[...], ((1,), (1,)))
    lines, sent_first = swap(0, sums[0:4] + sums[4:8] + sums[8:12])

    slots = slots_ref[...]
    lane, row = slots & 127, slots >> 7
    goal = []
    for c in range(4):
        value = jnp.zeros((groups, 128), jnp.float32)
        for h, line in enumerate(lines):
            spread = jnp.broadcast_to(line[c : c + 1, :], (groups, 128))
            value = jnp.where(row == h, lane_gather(spread, lane), value)
        goal.append(value)
    rate = friction * goal[3]

    def advance():
        for c in range(3):
            vel = at[3 + c]
            force = pair_strength * pull[c] + rate * (goal[c] - vel)
            vel = vel + time_step * force
            at[3 + c] = vel
            at[c] = at[c] + time_step * vel

    def one_step(step, carry):
        pair_forces()
        advance()
        return carry

    advance()
    lax.fori_loop(1, MD_STEPS, one_step, 0)
    at[6] = at[3] * at[3] + at[4] * at[4] + at[5] * at[5]
    for c in range(4):
        for part, piece in enumerate(thirds(at[3 + c])):
            for g in range(groups):
                data[pl.ds(part * 4 + c, 1), pl.ds(g * 128, 128)] = piece[g : g + 1, :]
    sums = by_hits(data[...], hits[...], ((1,), (1,)))
    moments = (sums[0:4] + sums[4:8] + sums[8:12]) / jnp.maximum(sums[12:13], 1.0)
    lines, sent_second = swap(1, moments)
    for h, line in enumerate(lines):
        for part, piece in enumerate(thirds(line)):
            table[pl.ds(part * 4, 4), pl.ds(h * 128, 128)] = piece
    sums = by_hits(table[...], placed[...], ((1,), (0,)))
    picked = sums[0:4] + sums[4:8] + sums[8:12]
    for c in range(4):
        for z in range(cz):
            cell_out[c, pl.ds(z, 1), :] = picked[c : c + 1, z * cx : (z + 1) * cx]
    for g in range(groups):
        here = pl.ds(g * 128, 128)
        for c in range(3):
            pos_out[pl.ds(c, 1), here] = at[c, pl.ds(g, 1), :]
            vel_out[pl.ds(c, 1), here] = at[3 + c, pl.ds(g, 1), :]
    sent_first()
    sent_second()
    for made in copies:
        made.wait_send()


def on_device(populations, relax, owners, positions, velocities, neighbours, atom_slots):
    cz, cx, ny = relax.shape
    n_slab = lax.axis_size("slab")
    n_md = lax.axis_size("md")
    devices = n_slab * n_md
    top = owners.shape[2]
    cap = cz * max(2, 2 * cx * top // devices)
    slots = devices * cap
    atoms, entries = neighbours.shape
    groups = atoms // 128
    cells = cz * cx
    vmem = pl.BlockSpec(memory_space=pltpu.VMEM)
    dma = pltpu.SemaphoreType.DMA
    return pl.pallas_call(
        functools.partial(coupled_kernel, n_slab, n_md),
        out_shape=(
            jax.ShapeDtypeStruct(populations.shape, jnp.float32),
            jax.ShapeDtypeStruct(positions.shape, jnp.float32),
            jax.ShapeDtypeStruct(velocities.shape, jnp.float32),
            jax.ShapeDtypeStruct((4, cz, cx), jnp.float32),
        ),
        in_specs=[vmem] * 7,
        out_specs=(vmem,) * 4,
        scratch_shapes=[
            pltpu.VMEM((LB_STEPS, 19, cz + 2, cx + 16, ny), jnp.float32),
            pltpu.VMEM((LB_STEPS, cz, 2, 8, ny), jnp.float32),
            pltpu.VMEM((LB_STEPS, cz + 2, 2, 8, ny), jnp.float32),
            pltpu.VMEM((4, cells, ny), jnp.float32),
            pltpu.VMEM((7, groups, 128), jnp.float32),
            pltpu.VMEM((3, groups, 128), jnp.float32),
            pltpu.VMEM((16, atoms), jnp.float32),
            pltpu.VMEM((slots, atoms), jnp.bfloat16),
            pltpu.VMEM((slots, cells), jnp.bfloat16),
            pltpu.VMEM((16, cells), jnp.float32),
            pltpu.VMEM((16, slots), jnp.float32),
            pltpu.VMEM((2, devices, 4, 128), jnp.float32),
            pltpu.VMEM((2, devices, 4, 128), jnp.float32),
            dma((LB_STEPS, 7 + 2 * cz)),
            dma((LB_STEPS, 7 + 2 * cz)),
            dma((2, devices)),
            dma((2, devices)),
        ],
        compiler_params=pltpu.CompilerParams(
            collective_id=0, has_side_effects=True, vmem_limit_bytes=40 * 1024 * 1024
        ),
        name="coupled",
    )(
        populations,
        relax,
        owners.reshape(cells, top).T,
        positions,
        velocities,
        neighbours.T,
        atom_slots.reshape(groups, 128),
    )


def solution(mesh):
    return jax.shard_map(
        on_device,
        mesh=mesh,
        in_specs=(
            P(None, "slab", "md", None),
            P("slab", "md", None),
            P("slab", "md", None),
            P(None, ("slab", "md")),
            P(None, ("slab", "md")),
            P(("slab", "md"), None),
            P(("slab", "md")),
        ),
        out_specs=(
            P(None, "slab", "md", None),
            P(None, ("slab", "md")),
            P(None, ("slab", "md")),
            P(None, "slab", "md"),
        ),
        check_vma=False,
    )
```
